32 devices in a mesh: rep: 4 (over x, y), dp: 8 (over z, core).
Axes of the slice: x: 2, y: 2, z: 4, core: 2. Of those that a mesh axis runs over, the one named last changes fastest.
Arguments:
- a: bfloat16 [32, 4, 8192, 768], P(('rep', 'dp')), parts along dimension 0
- g: bfloat16 [32, 4, 8192, 3072], P(('rep', 'dp')), parts along dimension 0
Outputs:
- output: bfloat16 [16, 768, 3072], P('rep'), parts along dimension 0
There are 4 independent parts. The reference program is written for one: setup_inputs(seed, part) draws one part's arguments, and reference() takes and returns one part's arrays. A program takes and returns all parts, laid end to end along the dimension named above; each array names one.
All inputs are finite; a program needn't handle non-finite values.
Results may differ from the reference program's by a relative error of at most 0.012.
Values are sent between devices in bfloat16 or wider.
A program may use at most 2 GiB of HBM per device.

```python
import jax
import jax.numpy as jnp
from jax import lax

DEVICES = 8
MATRICES = 4
TOKENS = 8192
D = 768
FF = 3072


def setup_inputs(seed: int = 0, part: int = 0) -> dict:
    ka, kg, ks = (jax.random.fold_in(k, part) for k in jax.random.split(jax.random.key(seed), 3))
    size = 2.0 ** jax.random.uniform(ks, (DEVICES, MATRICES, 1, 1), jnp.float32, -1.0, 1.0)
    a = jax.random.normal(ka, (DEVICES, MATRICES, TOKENS, D), jnp.float32)
    g = size * jax.random.normal(kg, (DEVICES, MATRICES, TOKENS, FF), jnp.float32) * (DEVICES * TOKENS) ** -0.5
    return {"a": a.astype(jnp.bfloat16), "g": g.astype(jnp.bfloat16)}


def reference(a, g):
    def take(so_far, one):
        return so_far + jnp.einsum("ntd,ntf->ndf", *one, preferred_element_type=jnp.float32), None

    return lax.scan(take, jnp.zeros((MATRICES, D, FF), jnp.float32), (a, g))[0].astype(jnp.bfloat16)
```

```python
import functools

import jax
import jax.numpy as jnp
from jax import lax
from jax.experimental import pallas as pl
from jax.experimental.pallas import tpu as pltpu
from jax.sharding import PartitionSpec as P

MESH = pl.DeviceIdType.MESH
FB = 512
UB = 256
NK = 2
GS = 3
R = 8
LC, LD, LE = 3, 5, 7
KEEP = 6


def kernel(
    a, g, out, abuf, gbuf, acc, own, sib_out, sib_in, low_out, low_in, pair_out, pair_in, fin,
    a_sem, g_sem, sib_s, sib_r, low_s, low_r, pair_s, pair_r, fin_s, fin_r, put_s, loc_s, put_r,
):
    n_mat, tokens, rows = a.shape
    cols = g.shape[2]
    kc, half = tokens // NK, rows // 2
    per_mat = cols // FB
    steps = n_mat * per_mat
    units, prods = 2 * steps, NK * steps

    me = lax.axis_index("dp")
    z, core = me // 2, me % 2
    middle = (z + 1) // 2 == 1
    sibling = z * 2 + 1 - core
    partner = (z + 1 - 2 * (z % 2)) * 2 + core
    across = (3 - z) * 2 + core
    mine = pl.multiple_of(core * half, half)
    other = pl.multiple_of((1 - core) * half, half)

    def a_copy(n, k):
        return pltpu.make_async_copy(
            a.at[n, pl.ds(k * kc, kc)], abuf.at[n % 2, pl.ds(k * kc, kc)], a_sem.at[n % 2, k]
        )

    def g_copy(t):
        n, j, k = t // (per_mat * NK), (t // NK) % per_mat, t % NK
        return pltpu.make_async_copy(
            g.at[n, pl.ds(pl.multiple_of(k * kc, kc), kc), pl.ds(pl.multiple_of(j * FB, FB), FB)],
            gbuf.at[t % GS],
            g_sem.at[t % GS],
        )

    def place(u):
        n, col = u // (2 * per_mat), u % (2 * per_mat)
        return out.at[n, pl.ds(mine, half), pl.ds(pl.multiple_of(col * UB, UB), UB)]

    def send(src, dst, s, r, device):
        return pltpu.make_async_remote_copy(
            src_ref=src, dst_ref=dst, send_sem=s, recv_sem=r, device_id={"dp": device}, device_id_type=MESH
        )

    def sib_copy(u):
        return send(sib_out.at[u % 4], sib_in.at[u % 4], sib_s.at[u % 4], sib_r.at[u % 4], sibling)

    def low_copy(u):
        return send(low_out.at[u % R], low_in.at[u % R], low_s.at[u % R], low_r.at[u % R], partner)

    def pair_copy(u):
        return send(pair_out.at[u % R], pair_in.at[u % R], pair_s.at[u % R], pair_r.at[u % R], across)

    def fin_copy(u):
        return send(fin.at[u % R], place(u), fin_s.at[u % R], fin_r.at[u % R], partner)

    def loc_copy(u):
        return pltpu.make_async_copy(fin.at[u % R], place(u), loc_s.at[u % R])

    def put_copy(u):
        return send(fin.at[u % R], place(u), put_s.at[u % R], put_r.at[u], sibling)

    def pass_copy(u):
        return send(place(u), place(u), put_s.at[u % R], put_r.at[u], sibling)

    for k in range(NK):
        a_copy(0, k).start()
        g_copy(jnp.int32(k)).start()

    barrier = pltpu.get_barrier_semaphore()
    for d in (sibling, partner):
        pl.semaphore_signal(barrier, inc=1, device_id={"dp": d}, device_id_type=MESH)

    @pl.when(middle)
    def _():
        pl.semaphore_signal(barrier, inc=1, device_id={"dp": across}, device_id_type=MESH)
        pl.semaphore_wait(barrier, 3)

    @pl.when(jnp.logical_not(middle))
    def _():
        pl.semaphore_wait(barrier, 2)

    def product(t):
        n, j, k = t // (per_mat * NK), (t // NK) % per_mat, t % NK

        @pl.when(t + GS - 1 < prods)
        def _():
            g_copy(t + GS - 1).start()

        @pl.when(j == 0)
        def _():
            a_copy(n, k).wait()

        @pl.when((j == 1) & (n < n_mat - 1))
        def _():
            a_copy(n + 1, k).start()

        g_copy(t).wait()
        d = lax.dot_general(
            abuf[n % 2, pl.ds(pl.multiple_of(k * kc, kc), kc), :],
            gbuf[t % GS],
            (((0,), (0,)), ((), ())),
            preferred_element_type=jnp.float32,
        )

        @pl.when(k == 0)
        def _():
            acc[...] = d

        @pl.when(k > 0)
        def _():
            acc[...] += d

    def stage_a(i):
        for h in range(2):
            u, c = 2 * i + h, slice(h * UB, (h + 1) * UB)
            sib_out[u % 4] = acc[pl.ds(other, half), c].astype(jnp.bfloat16)
            sib_copy(u).start()
        for h in range(2):
            u, c = 2 * i + h, slice(h * UB, (h + 1) * UB)
            own[u % R] = acc[pl.ds(mine, half), c]

    def stage_b(u):
        sib_copy(u).wait()
        total = own[u % R] + sib_in[u % 4].astype(jnp.float32)

        @pl.when(middle)
        def _():
            own[u % R] = total

        @pl.when(jnp.logical_not(middle))
        def _():
            low_out[u % R] = total.astype(jnp.bfloat16)
            low_copy(u).start()

    def stage_c(u):
        low_copy(u).wait_recv()
        pair_out[u % R] = (own[u % R] + low_in[u % R].astype(jnp.float32)).astype(jnp.bfloat16)
        pair_copy(u).start()

    def stage_d(u):
        @pl.when(u >= KEEP)
        def _():
            finish_d(u - KEEP)

        pair_copy(u).wait()
        fin[u % R] = (pair_out[u % R].astype(jnp.float32) + pair_in[u % R].astype(jnp.float32)).astype(jnp.bfloat16)
        fin_copy(u).start()
        put_copy(u).start()
        loc_copy(u).start()

    def finish_d(u):
        fin_copy(u).wait_send()
        put_copy(u).wait_send()
        loc_copy(u).wait()

    def stage_e(u):
        @pl.when(u >= KEEP)
        def _():
            pass_copy(u - KEEP).wait_send()

        low_copy(u).wait_send()
        fin_copy(u).wait_recv()
        pass_copy(u).start()

    def within(u):
        return (u >= 0) & (u < units)

    def tick(t, carry):
        i, k = t // 2, t % 2

        @pl.when(t < prods)
        def _():
            product(t)

            @pl.when(k == 1)
            def _():
                stage_a(i)

        @pl.when((k == 0) & within(t - 2))
        def _():
            stage_b(t - 2)
            stage_b(t - 1)

        @pl.when(middle & within(t - LC))
        def _():
            stage_c(t - LC)

        @pl.when(middle & within(t - LD))
        def _():
            stage_d(t - LD)

        @pl.when(jnp.logical_not(middle) & within(t - LE))
        def _():
            stage_e(t - LE)

        return carry

    lax.fori_loop(0, units + LE, tick, 0)

    @pl.when(middle)
    def _():
        lax.fori_loop(units - KEEP, units, lambda u, c: (finish_d(u), c)[1], 0)

    @pl.when(jnp.logical_not(middle))
    def _():
        lax.fori_loop(units - KEEP, units, lambda u, c: (pass_copy(u).wait_send(), c)[1], 0)

    def sibling_rows(u, c):
        put_copy(u).wait_recv()
        return c

    lax.fori_loop(0, units, sibling_rows, 0)


def local(a, g):
    a, g = a[0], g[0]
    n_mat, tokens, rows = a.shape
    cols = g.shape[2]
    kc, half = tokens // NK, rows // 2
    steps = n_mat * (cols // FB)
    bf, f32 = jnp.bfloat16, jnp.float32
    ring = pltpu.VMEM((R, half, UB), bf)
    four = pltpu.VMEM((4, half, UB), bf)
    dma = pltpu.SemaphoreType.DMA
    return pl.pallas_call(
        kernel,
        out_shape=jax.ShapeDtypeStruct((n_mat, rows, cols), bf),
        in_specs=[pl.BlockSpec(memory_space=pl.ANY)] * 2,
        out_specs=pl.BlockSpec(memory_space=pl.ANY),
        scratch_shapes=[
            pltpu.VMEM((2, tokens, rows), bf),
            pltpu.VMEM((GS, kc, FB), bf),
            pltpu.VMEM((rows, FB), f32),
            pltpu.VMEM((R, half, UB), f32),
            four, four, ring, ring, ring, ring, ring,
            dma((2, NK)), dma((GS,)),
            dma((4,)), dma((4,)), dma((R,)), dma((R,)), dma((R,)), dma((R,)),
            dma((R,)), dma((R,)), dma((R,)), dma((R,)), dma((2 * steps,)),
        ],
        compiler_params=pltpu.CompilerParams(
            collective_id=0, has_side_effects=True, vmem_limit_bytes=64_000_000
        ),
    )(a, g)


def solution(mesh):
    assert mesh.shape["dp"] == 8
    both = ("rep", "dp")
    return jax.shard_map(
        local, mesh=mesh, in_specs=(P(both), P(both)), out_specs=P("rep"), check_vma=False
    )
```

```python
import jax
import jax.numpy as jnp
from jax import lax
from jax.experimental import pallas as pl
from jax.experimental.pallas import tpu as pltpu
from jax.sharding import PartitionSpec as P

MESH = pl.DeviceIdType.MESH
FB = 512
UB = 256
Q = 2
R = 10
S = 8
LC, LD, LE = 2, 4, 9
KEEP = 6
NP = 6
PC, PD = 4, 7
OWN = 4


def kernel(
    a, g, out, abuf, gbuf, own, sib_out, sib_in, low, pair_out, pair_in, fin,
    a_sem, g_sem, sib_s, sib_r, low_s, low_r, pair_s, pair_r, fin_s, fin_r, put_s, loc_s, put_r,
):
    n_mat, tokens, rows = a.shape
    cols = g.shape[2]
    half = rows // 2
    part = half // Q
    per_mat = cols // FB
    steps = n_mat * per_mat
    units = 2 * steps

    me = lax.axis_index("dp")
    z, core = me // 2, me % 2
    middle = (z + 1) // 2 == 1
    end = jnp.logical_not(middle)
    sibling = z * 2 + 1 - core
    partner = (z + 1 - 2 * (z % 2)) * 2 + core
    across = (3 - z) * 2 + core
    mine = pl.multiple_of(core * half, half)

    def a_copy(n, s):
        first = pl.multiple_of((core * s + (1 - core) * (1 - s)) * half, half)
        return pltpu.make_async_copy(a.at[n, :, pl.ds(first, half)], abuf.at[s], a_sem.at[s])

    def g_copy(i):
        n, j = i // per_mat, i % per_mat
        return pltpu.make_async_copy(
            g.at[n, :, pl.ds(pl.multiple_of(j * FB, FB), FB)], gbuf.at[i % 2], g_sem.at[i % 2]
        )

    def g_first(h):
        c = pl.ds(h * UB, UB)
        return pltpu.make_async_copy(g.at[0, :, c], gbuf.at[0, :, c], g_sem.at[2 + h])

    def send(src, dst, s, r, device):
        return pltpu.make_async_remote_copy(
            src_ref=src, dst_ref=dst, send_sem=s, recv_sem=r, device_id={"dp": device}, device_id_type=MESH
        )

    def place(u, q):
        n, col = u // (2 * per_mat), u % (2 * per_mat)
        return out.at[n, pl.ds(mine + q * part, part), pl.ds(pl.multiple_of(col * UB, UB), UB)]

    def piece(q):
        return pl.ds(q * part, part)

    def sib_copy(u):
        return send(sib_out.at[u % 4], sib_in.at[u % 4], sib_s.at[u % 4], sib_r.at[u % 4], sibling)

    def low_copy(u, q):
        v = low.at[u % R, piece(q)]
        return send(v, v, low_s.at[u % R, q], low_r.at[u % R, q], partner)

    def pair_copy(u, q):
        return send(
            pair_out.at[u % S, piece(q)], pair_in.at[u % S, piece(q)],
            pair_s.at[u % S, q], pair_r.at[u % S, q], across,
        )

    def fin_copy(u, q):
        return send(fin.at[u % S, piece(q)], place(u, q), fin_s.at[u % S, q], fin_r.at[u % R, q], partner)

    def loc_copy(u, q):
        return pltpu.make_async_copy(fin.at[u % S, piece(q)], place(u, q), loc_s.at[u % S, q])

    def put_copy(u, q):
        return send(fin.at[u % S, piece(q)], place(u, q), put_s.at[u % S, q], put_r.at[u, q], sibling)

    def pass_copy(u, q):
        return send(place(u, q), place(u, q), put_s.at[u % S, q], put_r.at[u, q], sibling)

    a_copy(0, 0).start()
    g_first(0).start()
    a_copy(0, 1).start()
    g_first(1).start()

    barrier = pltpu.get_barrier_semaphore()
    for d in (sibling, partner):
        pl.semaphore_signal(barrier, inc=1, device_id={"dp": d}, device_id_type=MESH)

    @pl.when(middle)
    def _():
        pl.semaphore_signal(barrier, inc=1, device_id={"dp": across}, device_id_type=MESH)
        pl.semaphore_wait(barrier, 3)

    @pl.when(end)
    def _():
        pl.semaphore_wait(barrier, 2)

    def dot(x, y):
        return lax.dot_general(x, y, (((0,), (0,)), ((), ())), preferred_element_type=jnp.float32)

    def to_sibling(u, d):
        sib_out[u % 4] = d.astype(jnp.bfloat16)
        sib_copy(u).start()

    def chip_sum(u):
        sib_copy(u).wait()

        @pl.when(middle)
        def _():
            own[u % OWN] += sib_in[u % 4].astype(jnp.float32)

        @pl.when(end)
        def _():
            for q in range(Q):
                p = piece(q)
                low[u % R, p] = (own[u % OWN, p] + sib_in[u % 4, p].astype(jnp.float32)).astype(jnp.bfloat16)
                low_copy(u, q).start()

    def piece_c(u, q):
        p = piece(q)
        low_copy(u, q).wait_recv()
        pair_out[u % S, p] = (own[u % OWN, p] + low[u % R, p].astype(jnp.float32)).astype(jnp.bfloat16)
        pair_copy(u, q).start()

    def piece_d(u, q):
        @pl.when(u >= KEEP)
        def _():
            finish_piece(u - KEEP, q)

        p = piece(q)
        pair_copy(u, q).wait()
        fin[u % S, p] = (
            pair_out[u % S, p].astype(jnp.float32) + pair_in[u % S, p].astype(jnp.float32)
        ).astype(jnp.bfloat16)
        fin_copy(u, q).start()
        put_copy(u, q).start()
        loc_copy(u, q).start()

    def finish_piece(u, q):
        fin_copy(u, q).wait_send()
        put_copy(u, q).wait_send()
        loc_copy(u, q).wait()

    def finish_d(u):
        for q in range(Q):
            finish_piece(u, q)

    def finish_e(u):
        for q in range(Q):
            pass_copy(u, q).wait_send()

    def stage_e(u):
        @pl.when(u >= KEEP)
        def _():
            finish_e(u - KEEP)

        for q in range(Q):
            low_copy(u, q).wait_send()
            fin_copy(u, q).wait_recv()
            pass_copy(u, q).start()

    def within(u):
        return (u >= 0) & (u < units)

    def narrow(k, carry):
        u, s = k // 2, k % 2
        i, h = u // 2, u % 2

        @pl.when(k < 2)
        def _():
            a_copy(0, s).wait()

        @pl.when(k == 0)
        def _():
            g_first(0).wait()

        @pl.when(k == 2)
        def _():
            g_first(1).wait()

        @pl.when((h == 0) & (s == 0) & (i > 0))
        def _():
            g_copy(i).wait()

        d = dot(abuf[s], gbuf[i % 2, :, pl.ds(pl.multiple_of(h * UB, UB), UB)])

        @pl.when((h == 0) & (s == 0))
        def _():
            g_copy(i + 1).start()

        @pl.when(s == 0)
        def _():
            to_sibling(u, d)

        @pl.when(s == 1)
        def _():
            own[u % OWN] = d
            chip_sum(u)

        @pl.when(middle & (k >= PD) & (k < 2 * NP - 1))
        def _():
            piece_d((k - PD) // Q, (k - PD) % Q)

        @pl.when(middle & (k >= PC))
        def _():
            piece_c((k - PC) // Q, (k - PC) % Q)

        return carry

    lax.fori_loop(0, 2 * NP, narrow, 0)

    def tick(t, carry):
        i, k = t // 2, t % 2
        n, j = i // per_mat, i % per_mat

        @pl.when(i < steps)
        def _():
            @pl.when(j == 0)
            def _():
                a_copy(n, k).wait()

            @pl.when(k == 0)
            def _():
                g_copy(i).wait()

                @pl.when(i + 1 < steps)
                def _():
                    g_copy(i + 1).start()

            d = dot(abuf[k], gbuf[i % 2])

            @pl.when((j == per_mat - 1) & (n + 1 < n_mat))
            def _():
                a_copy(n + 1, k).start()

            @pl.when(k == 0)
            def _():
                for h in range(2):
                    to_sibling(2 * i + h, d[:, h * UB : (h + 1) * UB])

            @pl.when(k == 1)
            def _():
                for h in range(2):
                    own[(2 * i + h) % OWN] = d[:, h * UB : (h + 1) * UB]
                for h in range(2):
                    chip_sum(2 * i + h)

        for q in range(Q):

            @pl.when(middle & within(t - LD))
            def _():
                piece_d(t - LD, q)

            @pl.when(middle & within(t - LC))
            def _():
                piece_c(t - LC, q)

        @pl.when(end & within(t - LE))
        def _():
            stage_e(t - LE)

        return carry

    lax.fori_loop(NP, units + LE, tick, 0)

    def each(first, f):
        def step(u, c):
            f(u)
            return c

        lax.fori_loop(first, units, step, 0)

    @pl.when(middle)
    def _():
        each(units - KEEP, finish_d)

    @pl.when(end)
    def _():
        each(units - KEEP, finish_e)

    def sibling_rows(u):
        for q in range(Q):
            put_copy(u, q).wait_recv()

    each(0, sibling_rows)


def local(a, g):
    a, g = a[0], g[0]
    n_mat, tokens, rows = a.shape
    cols = g.shape[2]
    half = rows // 2
    steps = n_mat * (cols // FB)
    bf, f32 = jnp.bfloat16, jnp.float32

    def ring(slots, dtype=bf):
        return pltpu.VMEM((slots, half, UB), dtype)

    dma = pltpu.SemaphoreType.DMA
    return pl.pallas_call(
        kernel,
        out_shape=pltpu.VMEM((n_mat, rows, cols), bf),
        in_specs=[pl.BlockSpec(memory_space=pl.ANY)] * 2,
        out_specs=pl.BlockSpec(memory_space=pl.ANY),
        scratch_shapes=[
            pltpu.VMEM((2, tokens, half), bf),
            pltpu.VMEM((2, tokens, FB), bf),
            ring(OWN, f32), ring(4), ring(4), ring(R), ring(S), ring(S), ring(S),
            dma((2,)), dma((4,)),
            dma((4,)), dma((4,)), dma((R, Q)), dma((R, Q)), dma((S, Q)), dma((S, Q)),
            dma((S, Q)), dma((R, Q)), dma((S, Q)), dma((S, Q)), dma((2 * steps, Q)),
        ],
        compiler_params=pltpu.CompilerParams(
            collective_id=0, has_side_effects=True, vmem_limit_bytes=46_000_000
        ),
    )(a, g)


def solution(mesh):
    assert mesh.shape["dp"] == 8
    both = ("rep", "dp")
    return jax.shard_map(
        local, mesh=mesh, in_specs=(P(both), P(both)), out_specs=P("rep"), check_vma=False
    )
```

```python
import jax
import jax.numpy as jnp
from jax import lax
from jax.experimental import pallas as pl
from jax.experimental.pallas import tpu as pltpu
from jax.sharding import PartitionSpec as P

MESH = pl.DeviceIdType.MESH
FB = 512
UB = 256
Q = 2
R = 10
S = 8
LC, LD, LE = 2, 4, 9
KEEP = 6
NP = 6
PC, PD = 4, 7
OWN = 4


def kernel(
    a, g, out, abuf, gbuf, own, sib_out, sib_in, low, pair_out, pair_in, fin,
    a_sem, g_sem, sib_s, sib_r, low_s, low_r, pair_s, pair_r, fin_s, fin_r, put_s, loc_s, put_r,
):
    n_mat, tokens, rows = a.shape
    cols = g.shape[2]
    half = rows // 2
    part = half // Q
    per_mat = cols // FB
    steps = n_mat * per_mat
    units = 2 * steps

    me = lax.axis_index("dp")
    z, core = me // 2, me % 2
    middle = (z + 1) // 2 == 1
    end = jnp.logical_not(middle)
    sibling = z * 2 + 1 - core
    partner = (z + 1 - 2 * (z % 2)) * 2 + core
    across = (3 - z) * 2 + core
    mine = pl.multiple_of(core * half, half)

    def a_copy(n, s):
        first = pl.multiple_of((core * s + (1 - core) * (1 - s)) * half, half)
        return pltpu.make_async_copy(a.at[n, :, pl.ds(first, half)], abuf.at[s], a_sem.at[s])

    def g_copy(i):
        n, j = i // per_mat, i % per_mat
        return pltpu.make_async_copy(
            g.at[n, :, pl.ds(pl.multiple_of(j * FB, FB), FB)], gbuf.at[i % 2], g_sem.at[i % 2]
        )

    def g_first(h):
        c = pl.ds(h * UB, UB)
        return pltpu.make_async_copy(g.at[0, :, c], gbuf.at[0, :, c], g_sem.at[2 + h])

    def send(src, dst, s, r, device):
        return pltpu.make_async_remote_copy(
            src_ref=src, dst_ref=dst, send_sem=s, recv_sem=r, device_id={"dp": device}, device_id_type=MESH
        )

    def place(u, q):
        n, col = u // (2 * per_mat), u % (2 * per_mat)
        return out.at[n, pl.ds(mine + q * part, part), pl.ds(pl.multiple_of(col * UB, UB), UB)]

    def piece(q):
        return pl.ds(q * part, part)

    def sib_copy(u):
        return send(sib_out.at[u % 4], sib_in.at[u % 4], sib_s.at[u % 4], sib_r.at[u % 4], sibling)

    def low_copy(u, q):
        v = low.at[u % R, piece(q)]
        return send(v, v, low_s.at[u % R, q], low_r.at[u % R, q], partner)

    def pair_copy(u, q):
        return send(
            pair_out.at[u % S, piece(q)], pair_in.at[u % S, piece(q)],
            pair_s.at[u % S, q], pair_r.at[u % S, q], across,
        )

    def fin_copy(u, q):
        return send(fin.at[u % S, piece(q)], place(u, q), fin_s.at[u % S, q], fin_r.at[u % R, q], partner)

    def loc_copy(u, q):
        return pltpu.make_async_copy(fin.at[u % S, piece(q)], place(u, q), loc_s.at[u % S, q])

    def put_copy(u, q):
        return send(fin.at[u % S, piece(q)], place(u, q), put_s.at[u % S, q], put_r.at[u, q], sibling)

    def pass_copy(u, q):
        return send(place(u, q), place(u, q), put_s.at[u % S, q], put_r.at[u, q], sibling)

    a_copy(0, 0).start()
    g_first(0).start()
    a_copy(0, 1).start()
    g_first(1).start()

    barrier = pltpu.get_barrier_semaphore()
    for d in (sibling, partner):
        pl.semaphore_signal(barrier, inc=1, device_id={"dp": d}, device_id_type=MESH)

    @pl.when(middle)
    def _():
        pl.semaphore_signal(barrier, inc=1, device_id={"dp": across}, device_id_type=MESH)
        pl.semaphore_wait(barrier, 3)

    @pl.when(end)
    def _():
        pl.semaphore_wait(barrier, 2)

    def dot(x, y):
        return lax.dot_general(x, y, (((0,), (0,)), ((), ())), preferred_element_type=jnp.float32)

    def to_sibling(u, d):
        sib_out[u % 4] = d.astype(jnp.bfloat16)
        sib_copy(u).start()

    def chip_sum(u):
        sib_copy(u).wait()

        @pl.when(middle)
        def _():
            own[u % OWN] += sib_in[u % 4].astype(jnp.float32)

        @pl.when(end)
        def _():
            for q in range(Q):
                p = piece(q)
                low[u % R, p] = (own[u % OWN, p] + sib_in[u % 4, p].astype(jnp.float32)).astype(jnp.bfloat16)
                low_copy(u, q).start()

    def piece_c(u, q):
        p = piece(q)
        low_copy(u, q).wait_recv()
        pair_out[u % S, p] = (own[u % OWN, p] + low[u % R, p].astype(jnp.float32)).astype(jnp.bfloat16)
        pair_copy(u, q).start()

    def piece_d(u, q):
        @pl.when(u >= KEEP)
        def _():
            finish_piece(u - KEEP, q)

        p = piece(q)
        pair_copy(u, q).wait()
        fin[u % S, p] = (
            pair_out[u % S, p].astype(jnp.float32) + pair_in[u % S, p].astype(jnp.float32)
        ).astype(jnp.bfloat16)
        fin_copy(u, q).start()
        put_copy(u, q).start()
        loc_copy(u, q).start()

    def finish_piece(u, q):
        fin_copy(u, q).wait_send()
        put_copy(u, q).wait_send()
        loc_copy(u, q).wait()

    def finish_d(u):
        for q in range(Q):
            finish_piece(u, q)

    def finish_e(u):
        for q in range(Q):
            pass_copy(u, q).wait_send()

    def stage_e(u):
        @pl.when(u >= KEEP)
        def _():
            finish_e(u - KEEP)

        for q in range(Q):
            low_copy(u, q).wait_send()
            fin_copy(u, q).wait_recv()
            pass_copy(u, q).start()

    def within(u):
        return (u >= 0) & (u < units)

    def narrow(k, carry):
        u, s = k // 2, k % 2
        i, h = u // 2, u % 2

        @pl.when(k < 2)
        def _():
            a_copy(0, s).wait()

        @pl.when(k == 0)
        def _():
            g_first(0).wait()

        @pl.when(k == 2)
        def _():
            g_first(1).wait()

        @pl.when((h == 0) & (s == 0) & (i > 0))
        def _():
            g_copy(i).wait()

        d = dot(abuf[s], gbuf[i % 2, :, pl.ds(pl.multiple_of(h * UB, UB), UB)])

        @pl.when((h == 0) & (s == 0))
        def _():
            g_copy(i + 1).start()

        @pl.when(s == 0)
        def _():
            to_sibling(u, d)

        @pl.when(s == 1)
        def _():
            own[u % OWN] = d
            chip_sum(u)

        @pl.when(middle & (k >= PD))
        def _():
            piece_d((k - PD) // Q, (k - PD) % Q)

        @pl.when(middle & (k >= PC))
        def _():
            piece_c((k - PC) // Q, (k - PC) % Q)

        return carry

    lax.fori_loop(0, 2 * NP, narrow, 0)

    def tick(t, carry):
        i, k = t // 2, t % 2
        n, j = i // per_mat, i % per_mat

        @pl.when(i < steps)
        def _():
            @pl.when(j == 0)
            def _():
                a_copy(n, k).wait()

            @pl.when(k == 0)
            def _():
                g_copy(i).wait()

                @pl.when(i + 1 < steps)
                def _():
                    g_copy(i + 1).start()

            d = dot(abuf[k], gbuf[i % 2])

            @pl.when((j == per_mat - 1) & (n + 1 < n_mat))
            def _():
                a_copy(n + 1, k).start()

            @pl.when(k == 0)
            def _():
                for h in range(2):
                    to_sibling(2 * i + h, d[:, h * UB : (h + 1) * UB])

            @pl.when(k == 1)
            def _():
                for h in range(2):
                    own[(2 * i + h) % OWN] = d[:, h * UB : (h + 1) * UB]
                for h in range(2):
                    chip_sum(2 * i + h)

        @pl.when(middle & within(t - LD))
        def _():
            for q in range(Q // 2, Q):
                piece_d(t - LD, q)

        @pl.when(middle & within(t - LC))
        def _():
            for q in range(Q):
                piece_c(t - LC, q)

        @pl.when(middle & within(t - LD + 1))
        def _():
            for q in range(Q // 2):
                piece_d(t - LD + 1, q)

        @pl.when(end & within(t - LE))
        def _():
            stage_e(t - LE)

        return carry

    lax.fori_loop(NP, units + LE, tick, 0)

    def each(first, f):
        def step(u, c):
            f(u)
            return c

        lax.fori_loop(first, units, step, 0)

    @pl.when(middle)
    def _():
        each(units - KEEP, finish_d)

    @pl.when(end)
    def _():
        each(units - KEEP, finish_e)

    def sibling_rows(u):
        for q in range(Q):
            put_copy(u, q).wait_recv()

    each(0, sibling_rows)


def local(a, g):
    a, g = a[0], g[0]
    n_mat, tokens, rows = a.shape
    cols = g.shape[2]
    half = rows // 2
    steps = n_mat * (cols // FB)
    bf, f32 = jnp.bfloat16, jnp.float32

    def ring(slots, dtype=bf):
        return pltpu.VMEM((slots, half, UB), dtype)

    dma = pltpu.SemaphoreType.DMA
    return pl.pallas_call(
        kernel,
        out_shape=pltpu.VMEM((n_mat, rows, cols), bf),
        in_specs=[pl.BlockSpec(memory_space=pl.ANY)] * 2,
        out_specs=pl.BlockSpec(memory_space=pl.ANY),
        scratch_shapes=[
            pltpu.VMEM((2, tokens, half), bf),
            pltpu.VMEM((2, tokens, FB), bf),
            ring(OWN, f32), ring(4), ring(4), ring(R), ring(S), ring(S), ring(S),
            dma((2,)), dma((4,)),
            dma((4,)), dma((4,)), dma((R, Q)), dma((R, Q)), dma((S, Q)), dma((S, Q)),
            dma((S, Q)), dma((R, Q)), dma((S, Q)), dma((S, Q)), dma((2 * steps, Q)),
        ],
        compiler_params=pltpu.CompilerParams(
            collective_id=0, has_side_effects=True, vmem_limit_bytes=46_000_000
        ),
    )(a, g)


def solution(mesh):
    assert mesh.shape["dp"] == 8
    both = ("rep", "dp")
    return jax.shard_map(
        local, mesh=mesh, in_specs=(P(both), P(both)), out_specs=P("rep"), check_vma=False
    )
```
